32 devices in a mesh: row: 2 (over x), col: 4 (over y, core), depth: 4 (over z).
Axes of the slice: x: 2, y: 2, z: 4, core: 2. Of those that a mesh axis runs over, the one named last changes fastest.
Arguments:
- left_values: bfloat16 [96, 32, 4, 529], P('row', ('col', 'depth')), may hold values from -1.25 to 1.25
- left_columns: int32 [96, 32, 4], P('row', ('col', 'depth')), may hold values from 0 to 39, as said below
- right_values: bfloat16 [32, 40, 4, 3, 529], P(('col', 'depth'), 'row'), may hold values from -1.75 to 1.75
- right_columns: int32 [32, 40, 4, 3], P(('col', 'depth'), 'row'), may hold values from 0 to 31, as said below
Outputs:
- product_matrix: bfloat16 [2208, 2944], P('row', ('col', 'depth'))
The draws below stay inside these ranges and needn't reach their ends.
Inputs may be any that keep to these rules, and one draw needn't show every extreme that they name: `left_columns`: within one block row and panel the 4 entries are distinct. `right_columns`: within one block row and column tile the 3 entries are distinct.
All inputs are finite; a program needn't handle non-finite values.
Results may differ from the reference program's by a relative error of at most 0.001.
Values may be sent and summed in bfloat16 or wider, within the bound.
A program may use at most 192 MiB of HBM per device.

```python
import jax
import jax.numpy as jnp
from jax import lax

BLK = 23
PANEL = 40
KPAN = 32
SAP = 4
CT = 4
CTW = 32
SBP = 3
MB = 96
NB = 128


def distinct_columns(key, leading, choices, count):
    scores = jax.random.randint(key, leading + (choices,), 0, 1 << 20) * choices + jnp.arange(choices, dtype=jnp.int32)
    chosen = lax.top_k(scores, count)[1]
    return chosen.astype(jnp.int32)


def draw_left_columns(key, part):
    return distinct_columns(jax.random.fold_in(key, 11), (MB, KPAN), PANEL, SAP)


def draw_right_columns(key, part):
    return distinct_columns(jax.random.fold_in(key, 12), (KPAN, PANEL, CT), CTW, SBP)


def level_of(own_key, shape, pieces, smallest, high):
    factor_of, own = 1.0, jax.random.fold_in(own_key, 6)
    for dim, blocks in pieces:
        draws = jnp.exp(jax.random.uniform(jax.random.fold_in(own, dim), (blocks,), jnp.float32, smallest / len(pieces), high / len(pieces)))
        factor_of = factor_of * jnp.repeat(draws, shape[dim] // blocks).reshape([-1 if axis == dim else 1 for axis in range(len(shape))])
    return factor_of


def centred(rng, shape, width, most, pieces=(), held_as=jnp.bfloat16):
    loudness = level_of(rng, shape, pieces, -0.22, 0.18) if pieces else 1.0
    result = jax.random.normal(rng, shape, jnp.float32) * width * loudness
    return jnp.minimum(jnp.maximum(result, -most), most).astype(held_as)


def setup_inputs(seed: int = 0) -> dict:
    key_list = jax.random.split(jax.random.key(seed), 5)
    return {
        "left_values": centred(key_list[0], (MB, KPAN, SAP, BLK * BLK), BLK ** -0.5, 1.25, ((0, 2), (1, 16))),
        "left_columns": draw_left_columns(jax.random.fold_in(key_list[4], 71), 0),
        "right_values": centred(key_list[2], (KPAN, PANEL, CT, SBP, BLK * BLK), (SAP * SBP * KPAN // CTW) ** -0.5, 1.75, ((0, 16), (1, 2))),
        "right_columns": draw_right_columns(jax.random.fold_in(key_list[4], 71), 0),
    }


def reference(left_values, left_columns, right_values, right_columns):
    tile_base = (jnp.arange(CT, dtype=jnp.int32) * CTW)[None, None, :, None]
    row_ids = jnp.broadcast_to(jnp.arange(MB, dtype=jnp.int32)[:, None], (MB, SAP * CT * SBP))

    def panel_step(running, items):
        left_panel, left_cols, right_panel, right_cols = items
        chosen = right_panel[left_cols]
        chosen_cols = right_cols[left_cols] + tile_base
        left_mats = left_panel.astype(jnp.float32).reshape(MB, SAP, BLK, BLK)
        right_mats = chosen.astype(jnp.float32).reshape(MB, SAP, CT * SBP, BLK, BLK)
        partial_blocks = jnp.einsum("isab,isnbc->isnac", left_mats, right_mats, precision=lax.Precision.HIGHEST)
        partial_blocks = partial_blocks.reshape(MB, SAP * CT * SBP, BLK * BLK)
        running = running.at[row_ids, chosen_cols.reshape(MB, SAP * CT * SBP)].add(partial_blocks)
        return running, None

    start_blocks = jnp.zeros((MB, NB, BLK * BLK), jnp.float32)
    items = (jnp.transpose(left_values, (1, 0, 2, 3)), jnp.transpose(left_columns, (1, 0, 2)), right_values, right_columns)
    summed, unused = lax.scan(panel_step, start_blocks, items)
    dense = jnp.transpose(summed.reshape(MB, NB, BLK, BLK), (0, 2, 1, 3)).reshape(MB * BLK, NB * BLK)
    return dense.astype(jnp.bfloat16)
```

```python
import functools
import math

import jax
import jax.numpy as jnp
from jax import lax
from jax.experimental import pallas as pl
from jax.experimental.pallas import tpu as pltpu
from jax.sharding import PartitionSpec as P

CTW = 32


def lay_left(values, columns):
    rows, panels, slots, square = values.shape
    edge = math.isqrt(square)
    blocks = values.reshape(rows, panels, slots, edge, edge).transpose(1, 2, 4, 0, 3)
    blocks = blocks.reshape(panels, slots, edge, rows * edge)
    codes = jnp.repeat(columns.transpose(1, 2, 0).astype(jnp.bfloat16), edge, axis=2)
    return jnp.concatenate([blocks, codes[:, :, None, :]], axis=2)


def lay_right(values, columns):
    panels, rows, tiles, slots, square = values.shape
    edge = math.isqrt(square)
    blocks = values.reshape(panels, rows, tiles, slots, edge, edge).transpose(2, 0, 3, 5, 1, 4)
    blocks = jnp.pad(blocks, ((0, 0),) * 5 + ((0, 1),))
    blocks = blocks.reshape(tiles, panels, slots, edge, rows * (edge + 1))
    codes = jnp.repeat(columns.transpose(2, 0, 3, 1).astype(jnp.bfloat16), edge + 1, axis=3)
    return jnp.concatenate([blocks, codes[:, :, :, None, :]], axis=3)


def expand(values_ref, lead, slots, pad, count, out_ref, base):
    width = out_ref.shape[-1]
    lower = lax.broadcasted_iota(jnp.int32, (2 * pad, width), 0) >= pad
    shift = jnp.where(lower, 1.0, 0.0)
    doubled, codes = [], []
    for s in range(slots):
        one = values_ref[lead + (s,)].astype(jnp.float32)
        code = jnp.broadcast_to(one[pad - 1 : pad, :], (2 * pad, width)) - shift
        doubled.append(jnp.concatenate([one, one], axis=0).astype(jnp.bfloat16))
        codes.append(code.astype(jnp.bfloat16))
    for pair in range(count // 2):
        want = jnp.bfloat16(base + 2 * pair)
        filled = jnp.zeros((2 * pad, width), jnp.bfloat16)
        for s in range(slots):
            filled = jnp.where(codes[s] == want, doubled[s], filled)
        out_ref[2 * pad * pair : 2 * pad * (pair + 1), :] = filled


def product_kernel(pad, left_ref, right_ref, out_ref, left_dense, right_dense):
    @pl.when(pl.program_id(0) == 0)
    def _():
        out_ref[...] = jnp.zeros_like(out_ref)

    parts, _, slots_r = right_ref.shape[:3]
    slots_l = left_ref.shape[1]
    here = left_dense.shape[1] // pad
    for r in range(parts):
        expand(left_ref, (0,), slots_l, pad, here, left_dense.at[r], r * here)
        expand(right_ref, (r, 0), slots_r, pad, CTW, right_dense.at[r], 0)
    total = out_ref[...]
    for r in range(parts):
        total += jnp.dot(right_dense[r], left_dense[r], preferred_element_type=jnp.float32)
    out_ref[...] = total


def product(left, right, pad):
    panels, slots_l, _, m = left.shape
    parts, _, slots_r, _, k = right.shape
    n = CTW * pad
    return pl.pallas_call(
        functools.partial(product_kernel, pad),
        grid=(panels,),
        in_specs=[
            pl.BlockSpec((1, slots_l, pad, m), lambda p: (p, 0, 0, 0)),
            pl.BlockSpec((parts, 1, slots_r, pad, k), lambda p: (0, p, 0, 0, 0)),
        ],
        out_specs=pl.BlockSpec((n, m), lambda p: (0, 0)),
        out_shape=jax.ShapeDtypeStruct((n, m), jnp.float32),
        scratch_shapes=[pltpu.VMEM((parts, k, m), jnp.bfloat16), pltpu.VMEM((parts, n, k), jnp.bfloat16)],
        compiler_params=pltpu.CompilerParams(vmem_limit_bytes=56 << 20),
    )(left, right)


def body(left_values, left_columns, right_values, right_columns):
    pad = math.isqrt(left_values.shape[-1]) + 1
    left = lax.all_gather(lay_left(left_values, left_columns), "col", axis=0, tiled=True)
    right = lax.all_to_all(lay_right(right_values, right_columns), "col", 0, 0, tiled=True)
    tiles, panels, slots, _, k = right.shape
    right = lax.all_gather(right.reshape(tiles * panels, slots, pad, k), "row", axis=0)
    if right_values.shape[1] % 2:
        parts = right.shape[0]
        right = right.transpose(1, 2, 3, 0, 4).reshape(1, tiles * panels, slots, pad, parts * k)
    partial_sums = product(left, right, pad)
    result = lax.psum_scatter(partial_sums, "depth", scatter_dimension=0, tiled=True)
    rows, m = result.shape
    result = result.reshape(rows // pad, pad, m)[:, : pad - 1].reshape(rows // pad * (pad - 1), m)
    return result.T.astype(jnp.bfloat16)


def solution(mesh):
    placed = (
        P("row", ("col", "depth"), None, None),
        P("row", ("col", "depth"), None),
        P(("col", "depth"), "row", None, None, None),
        P(("col", "depth"), "row", None, None),
    )
    return jax.shard_map(
        body, mesh=mesh, in_specs=placed, out_specs=P("row", ("col", "depth")), check_vma=False
    )
```

```python
import functools
import math

import jax
import jax.numpy as jnp
from jax import lax
from jax.experimental import pallas as pl
from jax.experimental.pallas import tpu as pltpu
from jax.sharding import PartitionSpec as P

CTW = 32


def lay_left(values, columns):
    rows, panels, slots, square = values.shape
    edge = math.isqrt(square)
    blocks = values.reshape(rows, panels, slots, edge, edge).transpose(1, 2, 4, 0, 3)
    blocks = blocks.reshape(panels, slots, edge, rows * edge)
    codes = jnp.repeat(columns.transpose(1, 2, 0).astype(jnp.bfloat16), edge, axis=2)
    return jnp.concatenate([blocks, codes[:, :, None, :]], axis=2)


def lay_right(values, columns):
    panels, rows, tiles, slots, square = values.shape
    edge = math.isqrt(square)
    blocks = values.reshape(panels, rows, tiles, slots, edge, edge).transpose(2, 0, 3, 5, 1, 4)
    blocks = jnp.pad(blocks, ((0, 0),) * 5 + ((0, 1),))
    blocks = blocks.reshape(tiles, panels, slots, edge, rows * (edge + 1))
    codes = jnp.repeat(columns.transpose(2, 0, 3, 1).astype(jnp.bfloat16), edge + 1, axis=3)
    return jnp.concatenate([blocks, codes[:, :, :, None, :]], axis=3)


def expand(values_ref, lead, slots, pad, count, out_ref, base):
    width = out_ref.shape[-1]
    lower = lax.broadcasted_iota(jnp.int32, (2 * pad, width), 0) >= pad
    shift = jnp.where(lower, 1.0, 0.0)
    doubled, codes = [], []
    for s in range(slots):
        one = values_ref[lead + (s,)].astype(jnp.float32)
        code = jnp.broadcast_to(one[pad - 1 : pad, :], (2 * pad, width)) - shift
        doubled.append(jnp.concatenate([one, one], axis=0).astype(jnp.bfloat16))
        codes.append(code.astype(jnp.bfloat16))
    for pair in range(count // 2):
        want = jnp.bfloat16(base + 2 * pair)
        filled = jnp.zeros((2 * pad, width), jnp.bfloat16)
        for s in range(slots):
            filled = jnp.where(codes[s] == want, doubled[s], filled)
        out_ref[2 * pad * pair : 2 * pad * (pair + 1), :] = filled


def product_kernel(pad, left_ref, right_ref, out_ref, left_dense, right_dense):
    @pl.when(pl.program_id(0) == 0)
    def _():
        out_ref[...] = jnp.zeros_like(out_ref)

    parts, _, slots_r = right_ref.shape[:3]
    slots_l = left_ref.shape[1]
    here = left_dense.shape[1] // pad
    for r in range(parts):
        expand(left_ref, (0,), slots_l, pad, here, left_dense.at[r], r * here)
        expand(right_ref, (r, 0), slots_r, pad, CTW, right_dense.at[r], 0)
    total = out_ref[...]
    for r in range(parts):
        total += jnp.dot(right_dense[r], left_dense[r], preferred_element_type=jnp.float32)
    out_ref[...] = total


def product(left, right, pad):
    panels, slots_l, _, m = left.shape
    parts, _, slots_r, _, k = right.shape
    n = CTW * pad
    return pl.pallas_call(
        functools.partial(product_kernel, pad),
        grid=(panels,),
        in_specs=[
            pl.BlockSpec((1, slots_l, pad, m), lambda p: (p, 0, 0, 0)),
            pl.BlockSpec((parts, 1, slots_r, pad, k), lambda p: (0, p, 0, 0, 0)),
        ],
        out_specs=pl.BlockSpec((n, m), lambda p: (0, 0)),
        out_shape=jax.ShapeDtypeStruct((n, m), jnp.float32),
        scratch_shapes=[pltpu.VMEM((parts, k, m), jnp.bfloat16), pltpu.VMEM((parts, n, k), jnp.bfloat16)],
        compiler_params=pltpu.CompilerParams(vmem_limit_bytes=56 << 20),
    )(left, right)


def ring_kernel(streams, own_ref, out_ref, landed, send_sem, recv_sem):
    n = own_ref.shape[0]
    me = lax.axis_index("depth")
    after, before = lax.rem(me + 1, n), lax.rem(me + n - 1, n)
    barrier = pltpu.get_barrier_semaphore()
    for other in (before, after):
        pl.semaphore_signal(barrier, inc=1, device_id={"depth": other}, device_id_type=pl.DeviceIdType.MESH)
    pl.semaphore_wait(barrier, 2)

    rows = own_ref.shape[1] // streams
    spans = [pl.ds(rows * i, rows) for i in range(streams)]

    def hop(step, i, source):
        return pltpu.make_async_remote_copy(
            src_ref=source,
            dst_ref=landed.at[step, spans[i]],
            send_sem=send_sem.at[step, i],
            recv_sem=recv_sem.at[step, i],
            device_id={"depth": before if i % 2 else after},
            device_id_type=pl.DeviceIdType.MESH,
        )

    def chunk(step, i):
        return lax.rem(me + 1 + step, n) if i % 2 else lax.rem(me + 2 * n - 1 - step, n)

    hops = {}
    for i in range(streams):
        hops[0, i] = hop(0, i, own_ref.at[chunk(0, i), spans[i]])
        hops[0, i].start()
    for step in range(n - 1):
        for i in range(streams):
            hops[step, i].wait_recv()
            total = landed[step, spans[i], :] + own_ref[chunk(step + 1, i), spans[i], :]
            if step == n - 2:
                out_ref[spans[i], :] = total
            else:
                landed[step, spans[i], :] = total
                hops[step + 1, i] = hop(step + 1, i, landed.at[step, spans[i]])
                hops[step + 1, i].start()
    for each in hops.values():
        each.wait_send()


def ring_sum(partial_sums, n):
    rows, m = partial_sums.shape[0] // n, partial_sums.shape[1]
    streams = 4
    whole = pl.BlockSpec(memory_space=pltpu.VMEM)
    return pl.pallas_call(
        functools.partial(ring_kernel, streams),
        in_specs=[whole],
        out_specs=whole,
        out_shape=jax.ShapeDtypeStruct((rows, m), jnp.float32),
        scratch_shapes=[
            pltpu.VMEM((n - 1, rows, m), jnp.float32),
            pltpu.SemaphoreType.DMA((n - 1, streams)),
            pltpu.SemaphoreType.DMA((n - 1, streams)),
        ],
        compiler_params=pltpu.CompilerParams(collective_id=0, has_side_effects=True, vmem_limit_bytes=32 << 20),
    )(partial_sums.reshape(n, rows, m))


def body(depth, left_values, left_columns, right_values, right_columns):
    pad = math.isqrt(left_values.shape[-1]) + 1
    left = lay_left(left_values, left_columns)
    left, right_values = lax.optimization_barrier((left, right_values))
    left = lax.all_gather(left, "col", axis=0, tiled=True)
    left, right = lax.optimization_barrier((left, lay_right(right_values, right_columns)))
    right = lax.all_to_all(right, "col", 0, 0, tiled=True)
    tiles, panels, slots, _, k = right.shape
    right = lax.all_gather(right.reshape(tiles * panels, slots, pad, k), "row", axis=0)
    if right_values.shape[1] % 2:
        parts = right.shape[0]
        right = right.transpose(1, 2, 3, 0, 4).reshape(1, tiles * panels, slots, pad, parts * k)
    partial_sums = product(left, right, pad)
    result = ring_sum(partial_sums, depth)
    rows, m = result.shape
    result = result.reshape(rows // pad, pad, m)[:, : pad - 1].reshape(rows // pad * (pad - 1), m)
    return result.T.astype(jnp.bfloat16)


def solution(mesh):
    placed = (
        P("row", ("col", "depth"), None, None),
        P("row", ("col", "depth"), None),
        P(("col", "depth"), "row", None, None, None),
        P(("col", "depth"), "row", None, None),
    )
    return jax.shard_map(
        functools.partial(body, mesh.shape["depth"]), mesh=mesh, in_specs=placed, out_specs=P("row", ("col", "depth")), check_vma=False
    )
```

```python
import functools
import math

import jax
import jax.numpy as jnp
from jax import lax
from jax.experimental import pallas as pl
from jax.experimental.pallas import tpu as pltpu
from jax.sharding import PartitionSpec as P

CTW = 32


def lay_left(values, columns):
    rows, panels, slots, square = values.shape
    edge = math.isqrt(square)
    blocks = values.reshape(rows, panels, slots, edge, edge).transpose(1, 2, 4, 0, 3)
    blocks = blocks.reshape(panels, slots, edge, rows * edge)
    codes = jnp.repeat(columns.transpose(1, 2, 0).astype(jnp.bfloat16), edge, axis=2)
    return jnp.concatenate([blocks, codes[:, :, None, :]], axis=2)


def lay_right(values, columns):
    panels, rows, tiles, slots, square = values.shape
    edge = math.isqrt(square)
    blocks = values.reshape(panels, rows, tiles, slots, edge, edge).transpose(2, 0, 3, 5, 1, 4)
    blocks = jnp.pad(blocks, ((0, 0),) * 5 + ((0, 1),))
    blocks = blocks.reshape(tiles, panels, slots, edge, rows * (edge + 1))
    codes = jnp.repeat(columns.transpose(2, 0, 3, 1).astype(jnp.bfloat16), edge + 1, axis=3)
    return jnp.concatenate([blocks, codes[:, :, :, None, :]], axis=3)


def expand(values_ref, lead, slots, pad, count, out_ref, base):
    width = out_ref.shape[-1]
    lower = lax.broadcasted_iota(jnp.int32, (2 * pad, width), 0) >= pad
    shift = jnp.where(lower, 1.0, 0.0)
    doubled, codes = [], []
    for s in range(slots):
        one = values_ref[lead + (s,)].astype(jnp.float32)
        code = jnp.broadcast_to(one[pad - 1 : pad, :], (2 * pad, width)) - shift
        doubled.append(jnp.concatenate([one, one], axis=0).astype(jnp.bfloat16))
        codes.append(code.astype(jnp.bfloat16))
    for pair in range(count // 2):
        want = jnp.bfloat16(base + 2 * pair)
        filled = jnp.zeros((2 * pad, width), jnp.bfloat16)
        for s in range(slots):
            filled = jnp.where(codes[s] == want, doubled[s], filled)
        out_ref[2 * pad * pair : 2 * pad * (pair + 1), :] = filled


def product_kernel(pad, left_ref, right_ref, out_ref, left_dense, right_dense):
    @pl.when(pl.program_id(0) == 0)
    def _():
        out_ref[...] = jnp.zeros_like(out_ref)

    parts, _, slots_r = right_ref.shape[:3]
    slots_l = left_ref.shape[1]
    here = left_dense.shape[1] // pad
    for r in range(parts):
        expand(left_ref, (0,), slots_l, pad, here, left_dense.at[r], r * here)
        expand(right_ref, (r, 0), slots_r, pad, CTW, right_dense.at[r], 0)
    total = out_ref[...]
    for r in range(parts):
        total += jnp.dot(right_dense[r], left_dense[r], preferred_element_type=jnp.float32)
    out_ref[...] = total


def product(left, right, pad):
    panels, slots_l, _, m = left.shape
    parts, _, slots_r, _, k = right.shape
    n = CTW * pad
    return pl.pallas_call(
        functools.partial(product_kernel, pad),
        grid=(panels,),
        in_specs=[
            pl.BlockSpec((1, slots_l, pad, m), lambda p: (p, 0, 0, 0)),
            pl.BlockSpec((parts, 1, slots_r, pad, k), lambda p: (0, p, 0, 0, 0)),
        ],
        out_specs=pl.BlockSpec((n, m), lambda p: (0, 0)),
        out_shape=jax.ShapeDtypeStruct((n, m), jnp.float32),
        scratch_shapes=[pltpu.VMEM((parts, k, m), jnp.bfloat16), pltpu.VMEM((parts, n, k), jnp.bfloat16)],
        compiler_params=pltpu.CompilerParams(vmem_limit_bytes=56 << 20),
    )(left, right)


def gather_kernel(columns, rows, left_ref, right_ref, left_out, right_out, left_send, left_recv, tile_send, tile_recv, row_send, row_recv):
    me_col, me_row = lax.axis_index("col"), lax.axis_index("row")
    mesh_id = pl.DeviceIdType.MESH
    barrier = pltpu.get_barrier_semaphore()
    for d in range(1, columns):
        pl.semaphore_signal(barrier, inc=1, device_id={"col": lax.rem(me_col + d, columns)}, device_id_type=mesh_id)
    for d in range(1, rows):
        pl.semaphore_signal(barrier, inc=1, device_id={"row": lax.rem(me_row + d, rows)}, device_id_type=mesh_id)
    pl.semaphore_wait(barrier, columns + rows - 2)

    tile_hops, left_hops, row_hops = [], [], []
    for d in range(1, columns):
        other = lax.rem(me_col + d, columns)
        tile_hops.append(
            pltpu.make_async_remote_copy(
                src_ref=right_ref.at[other],
                dst_ref=right_out.at[me_row, me_col],
                send_sem=tile_send.at[d],
                recv_sem=tile_recv.at[d],
                device_id={"col": other},
                device_id_type=mesh_id,
            )
        )
        left_hops.append(
            pltpu.make_async_remote_copy(
                src_ref=left_ref,
                dst_ref=left_out.at[me_col],
                send_sem=left_send.at[d],
                recv_sem=left_recv.at[d],
                device_id={"col": other},
                device_id_type=mesh_id,
            )
        )

    def to_rows(d, source):
        slot = lax.rem(me_col + columns - d, columns)
        for e in range(1, rows):
            hop = pltpu.make_async_remote_copy(
                src_ref=source,
                dst_ref=right_out.at[me_row, slot],
                send_sem=row_send.at[e, d],
                recv_sem=row_recv.at[e, d],
                device_id={"row": lax.rem(me_row + e, rows)},
                device_id_type=mesh_id,
            )
            hop.start()
            row_hops.append(hop)

    for hop in tile_hops:
        hop.start()
    to_rows(0, right_ref.at[me_col])
    for hop in left_hops:
        hop.start()
    left_out[me_col] = left_ref[...]
    right_out[me_row, me_col] = right_ref[me_col]
    for d, hop in enumerate(tile_hops, 1):
        hop.wait_recv()
        to_rows(d, right_out.at[me_row, lax.rem(me_col + columns - d, columns)])
    for hop in left_hops + row_hops:
        hop.wait_recv()
    for hop in tile_hops + left_hops + row_hops:
        hop.wait_send()


def gather(left, right, columns, rows):
    whole = pl.BlockSpec(memory_space=pltpu.VMEM)
    dma = pltpu.SemaphoreType.DMA
    return pl.pallas_call(
        functools.partial(gather_kernel, columns, rows),
        in_specs=[whole, whole],
        out_specs=[whole, whole],
        out_shape=[
            jax.ShapeDtypeStruct((columns,) + left.shape, left.dtype),
            jax.ShapeDtypeStruct((rows,) + right.shape, right.dtype),
        ],
        scratch_shapes=[dma((columns,))] * 4 + [dma((rows, columns))] * 2,
        compiler_params=pltpu.CompilerParams(collective_id=1, has_side_effects=True, vmem_limit_bytes=32 << 20),
    )(left, right)


def ring_kernel(streams, own_ref, out_ref, landed, send_sem, recv_sem):
    n = own_ref.shape[0]
    me = lax.axis_index("depth")
    after, before = lax.rem(me + 1, n), lax.rem(me + n - 1, n)
    barrier = pltpu.get_barrier_semaphore()
    for other in (before, after):
        pl.semaphore_signal(barrier, inc=1, device_id={"depth": other}, device_id_type=pl.DeviceIdType.MESH)
    pl.semaphore_wait(barrier, 2)

    rows = own_ref.shape[1] // streams
    spans = [pl.ds(rows * i, rows) for i in range(streams)]

    def hop(step, i, source):
        return pltpu.make_async_remote_copy(
            src_ref=source,
            dst_ref=landed.at[step, spans[i]],
            send_sem=send_sem.at[step, i],
            recv_sem=recv_sem.at[step, i],
            device_id={"depth": before if i % 2 else after},
            device_id_type=pl.DeviceIdType.MESH,
        )

    def chunk(step, i):
        return lax.rem(me + 1 + step, n) if i % 2 else lax.rem(me + 2 * n - 1 - step, n)

    hops = {}
    for i in range(streams):
        hops[0, i] = hop(0, i, own_ref.at[chunk(0, i), spans[i]])
        hops[0, i].start()
    for step in range(n - 1):
        for i in range(streams):
            hops[step, i].wait_recv()
            total = landed[step, spans[i], :] + own_ref[chunk(step + 1, i), spans[i], :]
            if step == n - 2:
                out_ref[spans[i], :] = total
            else:
                landed[step, spans[i], :] = total
                hops[step + 1, i] = hop(step + 1, i, landed.at[step, spans[i]])
                hops[step + 1, i].start()
    for each in hops.values():
        each.wait_send()


def ring_sum(partial_sums, n):
    rows, m = partial_sums.shape[0] // n, partial_sums.shape[1]
    streams = 4
    whole = pl.BlockSpec(memory_space=pltpu.VMEM)
    return pl.pallas_call(
        functools.partial(ring_kernel, streams),
        in_specs=[whole],
        out_specs=whole,
        out_shape=jax.ShapeDtypeStruct((rows, m), jnp.float32),
        scratch_shapes=[
            pltpu.VMEM((n - 1, rows, m), jnp.float32),
            pltpu.SemaphoreType.DMA((n - 1, streams)),
            pltpu.SemaphoreType.DMA((n - 1, streams)),
        ],
        compiler_params=pltpu.CompilerParams(collective_id=0, has_side_effects=True, vmem_limit_bytes=32 << 20),
    )(partial_sums.reshape(n, rows, m))


def body(columns, rows, depth, left_values, left_columns, right_values, right_columns):
    pad = math.isqrt(left_values.shape[-1]) + 1
    left, right = gather(
        lay_left(left_values, left_columns), lay_right(right_values, right_columns), columns, rows
    )
    left = left.reshape((-1,) + left.shape[2:])
    right = right.reshape((rows, -1) + right.shape[3:])
    if right_values.shape[1] % 2:
        right = right.transpose(1, 2, 3, 0, 4)
        right = right.reshape((1,) + right.shape[:3] + (-1,))
    partial_sums = product(left, right, pad)
    result = ring_sum(partial_sums, depth)
    kept, m = result.shape
    result = result.reshape(kept // pad, pad, m)[:, : pad - 1].reshape(kept // pad * (pad - 1), m)
    return result.T.astype(jnp.bfloat16)


def solution(mesh):
    placed = (
        P("row", ("col", "depth"), None, None),
        P("row", ("col", "depth"), None),
        P(("col", "depth"), "row", None, None, None),
        P(("col", "depth"), "row", None, None),
    )
    return jax.shard_map(
        functools.partial(body, mesh.shape["col"], mesh.shape["row"], mesh.shape["depth"]), mesh=mesh, in_specs=placed, out_specs=P("row", ("col", "depth")), check_vma=False
    )
```

```python
import functools
import math

import jax
import jax.numpy as jnp
from jax import lax
from jax.experimental import pallas as pl
from jax.experimental.pallas import tpu as pltpu
from jax.sharding import PartitionSpec as P

CTW = 32


def lay_left(values, columns):
    rows, panels, slots, square = values.shape
    edge = math.isqrt(square)
    blocks = values.reshape(rows, panels, slots, edge, edge).transpose(1, 2, 4, 0, 3)
    blocks = blocks.reshape(panels, slots, edge, rows * edge)
    codes = jnp.repeat(columns.transpose(1, 2, 0).astype(jnp.bfloat16), edge, axis=2)
    return jnp.concatenate([blocks, codes[:, :, None, :]], axis=2)


def lay_right(values, columns):
    panels, rows, tiles, slots, square = values.shape
    edge = math.isqrt(square)
    blocks = values.reshape(panels, rows, tiles, slots, edge, edge).transpose(2, 0, 3, 5, 1, 4)
    blocks = jnp.pad(blocks, ((0, 0),) * 5 + ((0, 1),))
    blocks = blocks.reshape(tiles, panels, slots, edge, rows * (edge + 1))
    codes = jnp.repeat(columns.transpose(2, 0, 3, 1).astype(jnp.bfloat16), edge + 1, axis=3)
    return jnp.concatenate([blocks, codes[:, :, :, None, :]], axis=3)


def expand(values_ref, lead, slots, pad, count, out_ref, base):
    width = out_ref.shape[-1]
    lower = lax.broadcasted_iota(jnp.int32, (2 * pad, width), 0) >= pad
    shift = jnp.where(lower, 1.0, 0.0)
    doubled, codes = [], []
    for s in range(slots):
        one = values_ref[lead + (s,)].astype(jnp.float32)
        code = jnp.broadcast_to(one[pad - 1 : pad, :], (2 * pad, width)) - shift
        doubled.append(jnp.concatenate([one, one], axis=0).astype(jnp.bfloat16))
        codes.append(code.astype(jnp.bfloat16))
    for pair in range(count // 2):
        want = jnp.bfloat16(base + 2 * pair)
        filled = jnp.zeros((2 * pad, width), jnp.bfloat16)
        for s in range(slots):
            filled = jnp.where(codes[s] == want, doubled[s], filled)
        out_ref[2 * pad * pair : 2 * pad * (pair + 1), :] = filled


def product_kernel(pad, left_ref, right_ref, out_ref, left_dense, right_dense):
    @pl.when(pl.program_id(0) == 0)
    def _():
        out_ref[...] = jnp.zeros_like(out_ref)

    parts, _, slots_r = right_ref.shape[:3]
    slots_l = left_ref.shape[1]
    here = left_dense.shape[1] // pad
    for r in range(parts):
        expand(left_ref, (0,), slots_l, pad, here, left_dense.at[r], r * here)
        expand(right_ref, (r, 0), slots_r, pad, CTW, right_dense.at[r], 0)
    total = out_ref[...]
    for r in range(parts):
        total += jnp.dot(right_dense[r], left_dense[r], preferred_element_type=jnp.float32)
    out_ref[...] = total


def product(left, right, pad):
    panels, slots_l, _, m = left.shape
    parts, _, slots_r, _, k = right.shape
    n = CTW * pad
    return pl.pallas_call(
        functools.partial(product_kernel, pad),
        grid=(panels,),
        in_specs=[
            pl.BlockSpec((1, slots_l, pad, m), lambda p: (p, 0, 0, 0)),
            pl.BlockSpec((parts, 1, slots_r, pad, k), lambda p: (0, p, 0, 0, 0)),
        ],
        out_specs=pl.BlockSpec((n, m), lambda p: (0, 0)),
        out_shape=jax.ShapeDtypeStruct((n, m), jnp.float32),
        scratch_shapes=[pltpu.VMEM((parts, k, m), jnp.bfloat16), pltpu.VMEM((parts, n, k), jnp.bfloat16)],
        compiler_params=pltpu.CompilerParams(vmem_limit_bytes=56 << 20),
    )(left, right)


def gather_kernel(columns, rows, left_ref, right_ref, left_out, right_out, left_send, left_recv, tile_send, tile_recv, row_send, row_recv):
    me_col, me_row = lax.axis_index("col"), lax.axis_index("row")
    mesh_id = pl.DeviceIdType.MESH
    barrier = pltpu.get_barrier_semaphore()
    for d in range(1, columns):
        pl.semaphore_signal(barrier, inc=1, device_id={"col": lax.rem(me_col + d, columns)}, device_id_type=mesh_id)
    for d in range(1, rows):
        pl.semaphore_signal(barrier, inc=1, device_id={"row": lax.rem(me_row + d, rows)}, device_id_type=mesh_id)
    pl.semaphore_wait(barrier, columns + rows - 2)

    tile_hops, left_hops, row_hops = [], [], []
    for d in range(1, columns):
        other = lax.rem(me_col + d, columns)
        tile_hops.append(
            pltpu.make_async_remote_copy(
                src_ref=right_ref.at[other],
                dst_ref=right_out.at[me_row, me_col],
                send_sem=tile_send.at[d],
                recv_sem=tile_recv.at[d],
                device_id={"col": other},
                device_id_type=mesh_id,
            )
        )

    paired = columns % 2 == 0
    partner = me_col + 1 - 2 * lax.rem(me_col, 2)

    def left_hop(i, source, slot, other):
        return pltpu.make_async_remote_copy(
            src_ref=source,
            dst_ref=left_out.at[slot],
            send_sem=left_send.at[i],
            recv_sem=left_recv.at[i],
            device_id={"col": other},
            device_id_type=mesh_id,
        )

    strides = range(2, columns, 2) if paired else range(1, columns)
    left_hops = [left_hop(d, left_ref, me_col, lax.rem(me_col + d, columns)) for d in strides]
    passed = [left_hop(1, left_ref, me_col, partner)] if paired else []

    def to_rows(d, source):
        slot = lax.rem(me_col + columns - d, columns)
        for e in range(1, rows):
            hop = pltpu.make_async_remote_copy(
                src_ref=source,
                dst_ref=right_out.at[me_row, slot],
                send_sem=row_send.at[e, d],
                recv_sem=row_recv.at[e, d],
                device_id={"row": lax.rem(me_row + e, rows)},
                device_id_type=mesh_id,
            )
            hop.start()
            row_hops.append(hop)

    for hop in tile_hops:
        hop.start()
    to_rows(0, right_ref.at[me_col])
    for hop in left_hops + passed:
        hop.start()
    left_out[me_col] = left_ref[...]
    right_out[me_row, me_col] = right_ref[me_col]
    for d, hop in enumerate(tile_hops, 1):
        hop.wait_recv()
        to_rows(d, right_out.at[me_row, lax.rem(me_col + columns - d, columns)])
    for d, hop in zip(strides, left_hops):
        hop.wait_recv()
        if paired:
            slot = lax.rem(me_col + columns - d, columns)
            passed.append(left_hop(d + 1, left_out.at[slot], slot, partner))
            passed[-1].start()
    for hop in passed + row_hops:
        hop.wait_recv()
    for hop in tile_hops + left_hops + passed + row_hops:
        hop.wait_send()


def gather(left, right, columns, rows):
    whole = pl.BlockSpec(memory_space=pltpu.VMEM)
    dma = pltpu.SemaphoreType.DMA
    return pl.pallas_call(
        functools.partial(gather_kernel, columns, rows),
        in_specs=[whole, whole],
        out_specs=[whole, whole],
        out_shape=[
            jax.ShapeDtypeStruct((columns,) + left.shape, left.dtype),
            jax.ShapeDtypeStruct((rows,) + right.shape, right.dtype),
        ],
        scratch_shapes=[dma((columns,))] * 4 + [dma((rows, columns))] * 2,
        compiler_params=pltpu.CompilerParams(collective_id=1, has_side_effects=True, vmem_limit_bytes=32 << 20),
    )(left, right)


def ring_kernel(streams, own_ref, out_ref, landed, send_sem, recv_sem):
    n = own_ref.shape[0]
    me = lax.axis_index("depth")
    after, before = lax.rem(me + 1, n), lax.rem(me + n - 1, n)
    barrier = pltpu.get_barrier_semaphore()
    for other in (before, after):
        pl.semaphore_signal(barrier, inc=1, device_id={"depth": other}, device_id_type=pl.DeviceIdType.MESH)
    pl.semaphore_wait(barrier, 2)

    rows = own_ref.shape[1] // streams
    spans = [pl.ds(rows * i, rows) for i in range(streams)]

    def hop(step, i, source):
        return pltpu.make_async_remote_copy(
            src_ref=source,
            dst_ref=landed.at[step, spans[i]],
            send_sem=send_sem.at[step, i],
            recv_sem=recv_sem.at[step, i],
            device_id={"depth": before if i % 2 else after},
            device_id_type=pl.DeviceIdType.MESH,
        )

    def chunk(step, i):
        return lax.rem(me + 1 + step, n) if i % 2 else lax.rem(me + 2 * n - 1 - step, n)

    hops = {}
    for i in range(streams):
        hops[0, i] = hop(0, i, own_ref.at[chunk(0, i), spans[i]])
        hops[0, i].start()
    for step in range(n - 1):
        for i in range(streams):
            hops[step, i].wait_recv()
            total = landed[step, spans[i], :] + own_ref[chunk(step + 1, i), spans[i], :]
            if step == n - 2:
                out_ref[spans[i], :] = total
            else:
                landed[step, spans[i], :] = total
                hops[step + 1, i] = hop(step + 1, i, landed.at[step, spans[i]])
                hops[step + 1, i].start()
    for each in hops.values():
        each.wait_send()


def ring_sum(partial_sums, n):
    rows, m = partial_sums.shape[0] // n, partial_sums.shape[1]
    streams = 4
    whole = pl.BlockSpec(memory_space=pltpu.VMEM)
    return pl.pallas_call(
        functools.partial(ring_kernel, streams),
        in_specs=[whole],
        out_specs=whole,
        out_shape=jax.ShapeDtypeStruct((rows, m), jnp.float32),
        scratch_shapes=[
            pltpu.VMEM((n - 1, rows, m), jnp.float32),
            pltpu.SemaphoreType.DMA((n - 1, streams)),
            pltpu.SemaphoreType.DMA((n - 1, streams)),
        ],
        compiler_params=pltpu.CompilerParams(collective_id=0, has_side_effects=True, vmem_limit_bytes=32 << 20),
    )(partial_sums.reshape(n, rows, m))


def body(columns, rows, depth, left_values, left_columns, right_values, right_columns):
    pad = math.isqrt(left_values.shape[-1]) + 1
    left, right = gather(
        lay_left(left_values, left_columns), lay_right(right_values, right_columns), columns, rows
    )
    left = left.reshape((-1,) + left.shape[2:])
    right = right.reshape((rows, -1) + right.shape[3:])
    if right_values.shape[1] % 2:
        right = right.transpose(1, 2, 3, 0, 4)
        right = right.reshape((1,) + right.shape[:3] + (-1,))
    partial_sums = product(left, right, pad)
    result = ring_sum(partial_sums, depth)
    kept, m = result.shape
    result = result.reshape(kept // pad, pad, m)[:, : pad - 1].reshape(kept // pad * (pad - 1), m)
    return result.T.astype(jnp.bfloat16)


def solution(mesh):
    placed = (
        P("row", ("col", "depth"), None, None),
        P("row", ("col", "depth"), None),
        P(("col", "depth"), "row", None, None, None),
        P(("col", "depth"), "row", None, None),
    )
    return jax.shard_map(
        functools.partial(body, mesh.shape["col"], mesh.shape["row"], mesh.shape["depth"]), mesh=mesh, in_specs=placed, out_specs=P("row", ("col", "depth")), check_vma=False
    )
```
